32 devices in a mesh: batch: 1 (over z), row: 4 (over y), col: 8 (over x, core).
Axes of the slice: x: 4, y: 4, z: 1, core: 2. Of those that a mesh axis runs over, the one named last changes fastest.
The devices are a block of a 4x4x8 slice.
Arguments:
- spd_blocks: float32 [64, 128, 8192], P(('batch', 'row'), None, 'col')
Outputs:
- output: float32 [64, 128, 8192], P(('batch', 'row'), None, 'col')
All inputs are finite; a program needn't handle non-finite values.
Results may differ from the reference program's by a relative error of at most 0.001.
Values are sent between devices in bfloat16 or wider.
A program may use at most 768 MiB of HBM per device.

```python
import math
import jax
import jax.numpy as jnp
from jax import lax

BLOCK = 128
ORDER = 8192
ROW_DEVS = 4
COL_DEVS = 8

BLOCK_COUNT = ORDER // BLOCK


def to_logical(a_cyc):
    by_rows = a_cyc.reshape(ROW_DEVS, BLOCK_COUNT // ROW_DEVS, BLOCK, ORDER).transpose(1, 0, 2, 3)
    by_cols = by_rows.reshape(ORDER, COL_DEVS, BLOCK_COUNT // COL_DEVS, BLOCK).transpose(0, 2, 1, 3)
    return by_cols.reshape(ORDER, ORDER)


def to_cyclic(matrix):
    by_rows = matrix.reshape(BLOCK_COUNT // ROW_DEVS, ROW_DEVS, BLOCK, ORDER).transpose(1, 0, 2, 3)
    by_cols = by_rows.reshape(ORDER, BLOCK_COUNT // COL_DEVS, COL_DEVS, BLOCK).transpose(0, 2, 1, 3)
    return by_cols.reshape(BLOCK_COUNT, BLOCK, ORDER)


def setup_inputs(seed: int = 0, part: int = 0) -> dict:
    rng_key = jax.random.fold_in(jax.random.key(seed), part)
    gauss_draw = jax.random.normal(rng_key, (ORDER, ORDER), jnp.float32)
    sym_part = (gauss_draw + gauss_draw.T) * math.sqrt(0.5 / ORDER)
    matrix = (sym_part + 2.2 * jnp.eye(ORDER, dtype=jnp.float32)) * ORDER
    return {"spd_blocks": to_cyclic(matrix)}


def reference(spd_blocks):
    trailing = to_logical(spd_blocks)
    columns = []
    for step_idx in range(BLOCK_COUNT):
        diag_fac = jnp.tril(jnp.linalg.cholesky(trailing[:BLOCK, :BLOCK]))
        pieces = [jnp.zeros((step_idx * BLOCK, BLOCK), jnp.float32), diag_fac]
        if step_idx + 1 < BLOCK_COUNT:
            panel_f32 = lax.linalg.triangular_solve(diag_fac, trailing[BLOCK:, :BLOCK], left_side=False, lower=True, transpose_a=True)
            pieces.append(panel_f32)
            panel_b16 = panel_f32.astype(jnp.bfloat16)
            trailing = trailing[BLOCK:, BLOCK:] - jnp.dot(panel_b16, panel_b16.T, preferred_element_type=jnp.float32)
        columns.append(jnp.concatenate(pieces, axis=0))
    return to_cyclic(jnp.concatenate(columns, axis=1))
```

```python
import functools
import jax
import jax.numpy as jnp
from jax import lax
from jax.experimental import pallas as pl
from jax.experimental.pallas import tpu as pltpu
from jax.sharding import PartitionSpec as P

MESH = pl.DeviceIdType.MESH
F32 = jnp.float32
BF16 = jnp.bfloat16
SUB = 8
NT = (((1,), (1,)), ((), ()))


def chol_inv(blk):
    n = blk.shape[0]
    lane = lax.broadcasted_iota(jnp.int32, (SUB, n), 1)
    sub = lax.broadcasted_iota(jnp.int32, (SUB, n), 0)
    t = blk
    lout = jnp.zeros((n, n), F32)
    l_rows, inv_rows = [], []
    for p in range(n // SUB):
        base = p * SUB
        rows = n - base
        more = rows > SUB
        cols = [jnp.broadcast_to(t[:, base + m:base + m + 1], (rows, n)) for m in range(SUB)]
        c0 = [c[:SUB] for c in cols]
        inside = (lane >= base) & (lane < base + SUB)
        t0 = jnp.where(inside, jnp.where(lane == sub + base, 1.0, 0.0), t[:SUB])
        o0 = lout[:SUB]
        if more:
            c1 = [c[SUB:] for c in cols]
            lane1 = lax.broadcasted_iota(jnp.int32, (rows - SUB, n), 1)
            t1 = jnp.where((lane1 >= base) & (lane1 < base + SUB), 0.0, t[SUB:])
            o1 = lout[SUB:]
        for j in range(SUB):
            r = lax.rsqrt(jnp.broadcast_to(c0[j][j:j + 1], (SUB, n)))
            l0 = c0[j] * r
            l0m = jnp.where(sub > j, l0, 0.0)
            urow = jnp.broadcast_to(t0[j:j + 1], (SUB, n)) * r
            o0 = jnp.where((lane == base + j) & (sub >= j), l0, o0)
            t0 = jnp.where(sub == j, urow, t0 - l0m * urow)
            spl = {m: jnp.broadcast_to(c0[m][j:j + 1], (SUB, n)) * r for m in range(j + 1, SUB)}
            for m in range(j + 1, SUB):
                c0[m] = c0[m] - l0m * spl[m]
            if more:
                reps = (rows - SUB) // SUB
                wide = lambda v: jnp.concatenate([v] * reps, axis=0) if reps > 1 else v
                l1 = c1[j] * wide(r)
                o1 = jnp.where(lane1 == base + j, l1, o1)
                t1 = t1 - l1 * wide(urow)
                for m in range(j + 1, SUB):
                    c1[m] = c1[m] - l1 * wide(spl[m])
        inv_rows.append(jnp.where(lane < base + SUB, t0, 0.0))
        l_rows.append(o0)
        if more:
            t, lout = t1, o1
    return jnp.concatenate(l_rows, axis=0), jnp.concatenate(inv_rows, axis=0)


def split3(x):
    hi = x.astype(BF16)
    rest = x - hi.astype(F32)
    mid = rest.astype(BF16)
    lo = (rest - mid.astype(F32)).astype(BF16)
    return hi, mid, lo


def inv_operands(linv):
    w1, w2, w3 = split3(linv)
    top = jnp.concatenate([w2, w1], axis=1)
    bot = jnp.concatenate([w1, w2], axis=1)
    return jnp.concatenate([top, bot, jnp.concatenate([w3, w1], axis=1)], axis=0)


def solve_f32(x, ops):
    n = x.shape[1]
    x1, x2, x3 = split3(x)
    main = lax.dot_general(jnp.concatenate([x1, x2], axis=1), ops[:2 * n], NT, preferred_element_type=F32)
    tail = lax.dot_general(jnp.concatenate([x1, x3], axis=1), ops[2 * n:], NT, preferred_element_type=F32)
    return (tail + main[:, :n]) + main[:, n:]


def gather_kernel(dims, a_ref, sd_ref, *rest):
    s, blk, row_devs, col_devs, nr, nc = dims
    wide = nc > 0
    if wide:
        rp_ref, up_ref, own_sd, own_rp, own_up, send, recv, loc = rest
    else:
        own_sd, send, recv, loc = rest
    per = col_devs // row_devs
    r = lax.axis_index("row")
    c = lax.axis_index("col")
    cores = 2
    ring_x = col_devs // cores
    x, core = c // cores, c % cores
    yp, ym, y2 = (r + 1) % row_devs, (r + row_devs - 1) % row_devs, (r + 2) % row_devs
    xp = ((x + 1) % ring_x) * cores + core
    xm = ((x + ring_x - 1) % ring_x) * cores + core
    x2 = ((x + 2) % ring_x) * cores + core
    par = x * cores + (1 - core)
    pxp, pxm, px2 = ((x + 1) % ring_x) * cores + 1 - core, ((x + ring_x - 1) % ring_x) * cores + 1 - core, ((x + 2) % ring_x) * cores + 1 - core

    h = per * blk
    row0, col0 = s * h, s * blk
    a_sd = a_ref.at[pl.ds(row0, h), pl.ds(col0, blk)]
    sd_in = pltpu.make_async_copy(a_sd, own_sd, loc.at[0])
    sd_in.start()
    if wide:
        a_rp = a_ref.at[pl.ds(row0 + h, nr * blk), pl.ds(col0, blk)]
        a_up = a_ref.at[pl.ds(row0, h), pl.ds(col0 + blk, nc * blk)]
        rp_in = pltpu.make_async_copy(a_rp, own_rp, loc.at[1])
        up_in = pltpu.make_async_copy(a_up, own_up, loc.at[2])
        rp_in.start()
        up_in.start()

    barrier = pltpu.get_barrier_semaphore()
    for row, col in ((yp, c), (ym, c), (r, xp), (r, xm), (r, par)):
        pl.semaphore_signal(barrier, inc=1, device_id={"row": row, "col": col}, device_id_type=MESH)
    pl.semaphore_wait(barrier, 5)

    sent = []

    def put(idx, src, dst, row, col):
        cp = pltpu.make_async_remote_copy(src_ref=src, dst_ref=dst, send_sem=send.at[idx], recv_sem=recv.at[idx],
                                          device_id={"row": row, "col": col}, device_id_type=MESH)
        cp.start()
        sent.append(cp)

    def got(idx, dst):
        pltpu.make_async_remote_copy(src_ref=dst, dst_ref=dst, send_sem=send.at[idx], recv_sem=recv.at[idx],
                                     device_id={"row": r, "col": c}, device_id_type=MESH).wait_recv()

    put(0, a_sd, sd_ref.at[c, r], yp, c)
    put(1, a_sd, sd_ref.at[c, r], ym, c)
    if wide:
        put(4, a_rp, rp_ref.at[c], r, xp)
        put(5, a_rp, rp_ref.at[c], r, xm)
        put(6, a_rp, rp_ref.at[c], r, par)
        put(13, a_up, up_ref.at[r], yp, c)
        put(14, a_up, up_ref.at[r], ym, c)
    sd_in.wait()
    sd_out = pltpu.make_async_copy(own_sd, sd_ref.at[c, r], loc.at[0])
    sd_out.start()
    if wide:
        rp_in.wait()
        rp_out = pltpu.make_async_copy(own_rp, rp_ref.at[c], loc.at[1])
        rp_out.start()
        up_in.wait()
        up_out = pltpu.make_async_copy(own_up, up_ref.at[r], loc.at[2])
        up_out.start()
    half_y = h // 2
    lo_y, hi_y = pl.ds(0, half_y), pl.ds(half_y, half_y)
    got(0, sd_ref.at[c, ym])
    put(2, sd_ref.at[c, ym, lo_y], sd_ref.at[c, ym, lo_y], yp, c)
    got(1, sd_ref.at[c, yp])
    put(3, sd_ref.at[c, yp, hi_y], sd_ref.at[c, yp, hi_y], ym, c)
    sd_out.wait()
    got(2, sd_ref.at[c, y2, lo_y])
    got(3, sd_ref.at[c, y2, hi_y])
    put(17, sd_ref.at[c], sd_ref.at[c], r, xp)
    put(18, sd_ref.at[c], sd_ref.at[c], r, xm)
    put(19, sd_ref.at[c], sd_ref.at[c], r, par)

    def ring_x_rest(first, ref, lo, hi):
        got(first, ref.at[xm])
        put(first + 3, ref.at[xm].at[lo], ref.at[xm].at[lo], r, xp)
        put(first + 5, ref.at[xm], ref.at[xm], r, par)
        got(first + 1, ref.at[xp])
        put(first + 4, ref.at[xp].at[hi], ref.at[xp].at[hi], r, xm)
        put(first + 6, ref.at[xp], ref.at[xp], r, par)

    def ring_x_end(first, ref, lo, hi):
        got(first + 3, ref.at[x2].at[lo])
        put(first + 7, ref.at[x2].at[lo], ref.at[x2].at[lo], r, par)
        got(first + 4, ref.at[x2].at[hi])
        put(first + 8, ref.at[x2].at[hi], ref.at[x2].at[hi], r, par)

    def ring_x_partner(first, ref, lo, hi):
        got(first + 2, ref.at[par])
        got(first + 5, ref.at[pxm])
        got(first + 6, ref.at[pxp])
        got(first + 7, ref.at[px2].at[lo])
        got(first + 8, ref.at[px2].at[hi])

    half_r = row_devs // 2
    sd_halves = (pl.ds(0, half_r), pl.ds(half_r, half_r))
    if wide:
        half_p = nr * blk // 2
        rp_halves = (pl.ds(0, half_p), pl.ds(half_p, half_p))
        ring_x_rest(4, rp_ref, *rp_halves)
        got(13, up_ref.at[ym])
        put(15, up_ref.at[ym, lo_y], up_ref.at[ym, lo_y], yp, c)
        got(14, up_ref.at[yp])
        put(16, up_ref.at[yp, hi_y], up_ref.at[yp, hi_y], ym, c)
    ring_x_rest(17, sd_ref, *sd_halves)
    if wide:
        ring_x_end(4, rp_ref, *rp_halves)
    ring_x_end(17, sd_ref, *sd_halves)
    if wide:
        got(15, up_ref.at[y2, lo_y])
        got(16, up_ref.at[y2, hi_y])
        ring_x_partner(4, rp_ref, *rp_halves)
        rp_out.wait()
        up_out.wait()
    ring_x_partner(17, sd_ref, *sd_halves)
    for cp in sent:
        cp.wait_send()


def gather(a2, s, blk, row_devs, col_devs, nr, nc):
    per = col_devs // row_devs
    h = per * blk
    outs = [jax.ShapeDtypeStruct((col_devs, row_devs, h, blk), F32)]
    scratch = [pltpu.VMEM((h, blk), F32)]
    if nc:
        outs += [jax.ShapeDtypeStruct((col_devs, nr * blk, blk), F32), jax.ShapeDtypeStruct((row_devs, h, nc * blk), F32)]
        scratch += [pltpu.VMEM((nr * blk, blk), F32), pltpu.VMEM((h, nc * blk), F32)]
    anyspec = pl.BlockSpec(memory_space=pl.ANY)
    return pl.pallas_call(
        functools.partial(gather_kernel, (s, blk, row_devs, col_devs, nr, nc)),
        out_shape=outs,
        in_specs=[anyspec],
        out_specs=[anyspec] * len(outs),
        scratch_shapes=scratch + [pltpu.SemaphoreType.DMA((26,)), pltpu.SemaphoreType.DMA((26,)), pltpu.SemaphoreType.DMA((3,))],
        compiler_params=pltpu.CompilerParams(collective_id=s, has_side_effects=True),
        name=f"gather_{s}",
    )(a2)


def factor_kernel(dims, a_ref, sd_hbm, *rest):
    s, blk, row_devs, col_devs, nr, nc = dims
    wide = nc > 0
    if wide:
        rp_hbm, up_hbm, out_ref, sd, dblk, linv, bsd, zero, sems, pan, up, w, bpan = rest
    else:
        out_ref, sd, dblk, linv, bsd, zero, sems = rest
    per = col_devs // row_devs
    h = per * blk
    row0, col0 = s * h, s * blk
    r = lax.axis_index("row")
    c = lax.axis_index("col")
    sd_in = pltpu.make_async_copy(sd_hbm, sd, sems.at[0])
    sd_in.start()
    if wide:
        up_in = pltpu.make_async_copy(up_hbm, up, sems.at[2])
        up_in.start()
        rp_in = pltpu.make_async_copy(rp_hbm, pan.at[:, pl.ds(0, nr * blk)], sems.at[1])
        rp_in.start()
        w_in = pltpu.make_async_copy(a_ref.at[pl.ds(row0 + h, nr * blk), pl.ds(col0 + blk, nc * blk)], w, sems.at[3])
        w_in.start()
        zero[...] = jnp.zeros_like(zero)
        z_out = pltpu.make_async_copy(zero, out_ref.at[pl.ds(row0, h), pl.ds(col0 + blk, nc * blk)], sems.at[4])
        z_out.start()
    sd_in.wait()

    def at(j, k):
        return (k, j % row_devs, pl.ds((j // row_devs) * blk, blk))

    dblk[...] = sd[at(0, 0)]

    @pl.loop(0, col_devs)
    def _(k):
        lfac, inv = chol_inv(dblk[...])
        dblk[...] = lfac
        linv[k] = inv_operands(inv)
        for kk in range(col_devs):
            @pl.when(k == kk)
            def _():
                sd[at(kk, kk)] = dblk[...]
                if kk + 1 < col_devs:
                    ops = linv[kk]
                    below = jnp.concatenate([sd[at(j, kk)] for j in range(kk + 1, col_devs)], axis=0)
                    low = solve_f32(below, ops)
                    for j in range(kk + 1, col_devs):
                        sd[at(j, kk)] = low[(j - kk - 1) * blk:(j - kk) * blk]
                    bsd[(kk + 1) * blk:, kk * blk:(kk + 1) * blk] = low.astype(BF16)
                    upd = lax.dot_general(bsd[(kk + 1) * blk:, :(kk + 1) * blk], bsd[(kk + 1) * blk:(kk + 2) * blk, :(kk + 1) * blk], NT,
                                          preferred_element_type=F32)
                    dblk[...] = sd[at(kk + 1, kk + 1)] - upd[:blk]
                    for j in range(kk + 2, col_devs):
                        sd[at(j, kk + 1)] = sd[at(j, kk + 1)] - upd[(j - kk - 1) * blk:(j - kk) * blk]

    for tt in range(per):
        own = sd[c, r, pl.ds(tt * blk, blk)]
        sd[c, r, pl.ds(tt * blk, blk)] = jnp.where(tt * row_devs + r >= c, own, jnp.zeros_like(own))
    d_out = pltpu.make_async_copy(sd.at[c, r], out_ref.at[pl.ds(row0, h), pl.ds(col0, blk)], sems.at[0])
    d_out.start()
    if wide:
        up_in.wait()
        rp_in.wait()
        for k in range(col_devs):
            for jj in range(nc):
                pan[k, pl.ds((nr + jj) * blk, blk)] = up[k % row_devs, pl.ds((k // row_devs) * blk, blk), pl.ds(jj * blk, blk)].T
        for k in range(col_devs):
            ops = linv[k]

            @pl.loop(0, nr + nc)
            def _(i):
                sl = pl.ds(pl.multiple_of(i * blk, blk), blk)
                cur = pan[k, sl]
                if k:
                    cur = cur - lax.dot_general(bpan[sl, :k * blk], bsd[k * blk:(k + 1) * blk, :k * blk], NT, preferred_element_type=F32)
                low = solve_f32(cur, ops)
                pan[k, sl] = low
                bpan[sl, k * blk:(k + 1) * blk] = low.astype(BF16)
        l_out = pltpu.make_async_copy(pan.at[c, pl.ds(0, nr * blk)], out_ref.at[pl.ds(row0 + h, nr * blk), pl.ds(col0, blk)], sems.at[1])
        l_out.start()
        w_in.wait()

        @pl.loop(0, nr // 2)
        def _(i):
            sl = pl.ds(pl.multiple_of(i * 2 * blk, 2 * blk), 2 * blk)
            w[sl] = w[sl] - lax.dot_general(bpan[sl], bpan[nr * blk:], NT, preferred_element_type=F32)
        w_out = pltpu.make_async_copy(w, out_ref.at[pl.ds(row0 + h, nr * blk), pl.ds(col0 + blk, nc * blk)], sems.at[3])
        w_out.start()
        w_out.wait()
        l_out.wait()
        z_out.wait()
    d_out.wait()


def factor(a2, parts, s, blk, row_devs, col_devs, nr, nc):
    per = col_devs // row_devs
    h = per * blk
    anyspec = pl.BlockSpec(memory_space=pl.ANY)
    scratch = [
        pltpu.VMEM((col_devs, row_devs, h, blk), F32),
        pltpu.VMEM((blk, blk), F32),
        pltpu.VMEM((col_devs, 3 * blk, 2 * blk), BF16),
        pltpu.VMEM((col_devs * blk, col_devs * blk), BF16),
        pltpu.VMEM((h, max(nc, 1) * blk), F32),
        pltpu.SemaphoreType.DMA((5,)),
    ]
    if nc:
        scratch += [
            pltpu.VMEM((col_devs, (nr + nc) * blk, blk), F32),
            pltpu.VMEM((row_devs, h, nc * blk), F32),
            pltpu.VMEM((nr * blk, nc * blk), F32),
            pltpu.VMEM(((nr + nc) * blk, col_devs * blk), BF16),
        ]
    return pl.pallas_call(
        functools.partial(factor_kernel, (s, blk, row_devs, col_devs, nr, nc)),
        out_shape=jax.ShapeDtypeStruct(a2.shape, F32),
        in_specs=[anyspec] * (1 + len(parts)),
        out_specs=anyspec,
        scratch_shapes=scratch,
        input_output_aliases={} if s == 0 else {0: 0},
        compiler_params=pltpu.CompilerParams(vmem_limit_bytes=60 * 1024 * 1024),
        name=f"factor_{s}",
    )(a2, *parts)


def solution(mesh):
    row_devs = mesh.shape["row"]
    col_devs = mesh.shape["col"]
    per = col_devs // row_devs

    def factor_local(a_loc):
        row_blocks, blk, local_cols = a_loc.shape
        col_blocks = local_cols // blk
        a2 = a_loc.reshape(row_blocks * blk, local_cols)
        for s in range(col_blocks):
            nr, nc = row_blocks - per * (s + 1), col_blocks - s - 1
            parts = gather(a2, s, blk, row_devs, col_devs, nr, nc)
            a2 = factor(a2, parts, s, blk, row_devs, col_devs, nr, nc)
        return a2.reshape(row_blocks, blk, local_cols)

    spec = P(("batch", "row"), None, "col")
    return jax.shard_map(factor_local, mesh=mesh, in_specs=(spec,), out_specs=spec, check_vma=False)
```

```python
import functools
import jax
import jax.numpy as jnp
from jax import lax
from jax.experimental import pallas as pl
from jax.experimental.pallas import tpu as pltpu
from jax.sharding import PartitionSpec as P

MESH = pl.DeviceIdType.MESH
F32 = jnp.float32
BF16 = jnp.bfloat16
SUB = 8
NT = (((1,), (1,)), ((), ()))


def chol_inv(blk):
    n = blk.shape[0]
    lane = lax.broadcasted_iota(jnp.int32, (SUB, n), 1)
    sub = lax.broadcasted_iota(jnp.int32, (SUB, n), 0)
    t = blk
    lout = jnp.zeros((n, n), F32)
    l_rows, inv_rows = [], []
    for p in range(n // SUB):
        base = p * SUB
        rows = n - base
        more = rows > SUB
        cols = [jnp.broadcast_to(t[:, base + m:base + m + 1], (rows, n)) for m in range(SUB)]
        c0 = [c[:SUB] for c in cols]
        inside = (lane >= base) & (lane < base + SUB)
        t0 = jnp.where(inside, jnp.where(lane == sub + base, 1.0, 0.0), t[:SUB])
        o0 = lout[:SUB]
        if more:
            c1 = [c[SUB:] for c in cols]
            lane1 = lax.broadcasted_iota(jnp.int32, (rows - SUB, n), 1)
            t1 = jnp.where((lane1 >= base) & (lane1 < base + SUB), 0.0, t[SUB:])
            o1 = lout[SUB:]
        for j in range(SUB):
            r = lax.rsqrt(jnp.broadcast_to(c0[j][j:j + 1], (SUB, n)))
            l0 = c0[j] * r
            l0m = jnp.where(sub > j, l0, 0.0)
            urow = jnp.broadcast_to(t0[j:j + 1], (SUB, n)) * r
            o0 = jnp.where((lane == base + j) & (sub >= j), l0, o0)
            t0 = jnp.where(sub == j, urow, t0 - l0m * urow)
            spl = {m: jnp.broadcast_to(c0[m][j:j + 1], (SUB, n)) * r for m in range(j + 1, SUB)}
            for m in range(j + 1, SUB):
                c0[m] = c0[m] - l0m * spl[m]
            if more:
                reps = (rows - SUB) // SUB
                wide = lambda v: jnp.concatenate([v] * reps, axis=0) if reps > 1 else v
                l1 = c1[j] * wide(r)
                o1 = jnp.where(lane1 == base + j, l1, o1)
                t1 = t1 - l1 * wide(urow)
                for m in range(j + 1, SUB):
                    c1[m] = c1[m] - l1 * wide(spl[m])
        inv_rows.append(jnp.where(lane < base + SUB, t0, 0.0))
        l_rows.append(o0)
        if more:
            t, lout = t1, o1
    return jnp.concatenate(l_rows, axis=0), jnp.concatenate(inv_rows, axis=0)


def split3(x):
    hi = x.astype(BF16)
    rest = x - hi.astype(F32)
    mid = rest.astype(BF16)
    lo = (rest - mid.astype(F32)).astype(BF16)
    return hi, mid, lo


def inv_operands(linv):
    w1, w2, w3 = split3(linv)
    top = jnp.concatenate([w2, w1], axis=1)
    bot = jnp.concatenate([w1, w2], axis=1)
    return jnp.concatenate([top, bot, jnp.concatenate([w3, w1], axis=1)], axis=0)


def solve_f32(x, ops):
    n = x.shape[1]
    x1, x2, x3 = split3(x)
    main = lax.dot_general(jnp.concatenate([x1, x2], axis=1), ops[:2 * n], NT, preferred_element_type=F32)
    tail = lax.dot_general(jnp.concatenate([x1, x3], axis=1), ops[2 * n:], NT, preferred_element_type=F32)
    return (tail + main[:, :n]) + main[:, n:]


def gather_kernel(dims, a_ref, sd_ref, *rest):
    s, blk, row_devs, col_devs, nr, nc = dims
    wide = nc > 0
    if wide:
        rp_ref, up_ref, own_sd, own_rp, own_up, send, recv, loc = rest
    else:
        own_sd, send, recv, loc = rest
    per = col_devs // row_devs
    r = lax.axis_index("row")
    c = lax.axis_index("col")
    cores = 2
    ring_x = col_devs // cores
    x, core = c // cores, c % cores
    yp, ym, y2 = (r + 1) % row_devs, (r + row_devs - 1) % row_devs, (r + 2) % row_devs
    xp = ((x + 1) % ring_x) * cores + core
    xm = ((x + ring_x - 1) % ring_x) * cores + core
    x2 = ((x + 2) % ring_x) * cores + core
    par = x * cores + (1 - core)
    pxp, pxm, px2 = ((x + 1) % ring_x) * cores + 1 - core, ((x + ring_x - 1) % ring_x) * cores + 1 - core, ((x + 2) % ring_x) * cores + 1 - core

    h = per * blk
    row0, col0 = s * h, s * blk
    a_sd = a_ref.at[pl.ds(row0, h), pl.ds(col0, blk)]
    sd_in = pltpu.make_async_copy(a_sd, own_sd, loc.at[0])
    sd_in.start()
    if wide:
        a_rp = a_ref.at[pl.ds(row0 + h, nr * blk), pl.ds(col0, blk)]
        a_up = a_ref.at[pl.ds(row0, h), pl.ds(col0 + blk, nc * blk)]
        rp_in = pltpu.make_async_copy(a_rp, own_rp, loc.at[1])
        up_in = pltpu.make_async_copy(a_up, own_up, loc.at[2])
        rp_in.start()
        up_in.start()

    barrier = pltpu.get_barrier_semaphore()
    for row, col in ((yp, c), (ym, c), (r, xp), (r, xm), (r, par)):
        pl.semaphore_signal(barrier, inc=1, device_id={"row": row, "col": col}, device_id_type=MESH)
    pl.semaphore_wait(barrier, 5)

    sent = []

    def put(idx, src, dst, row, col):
        cp = pltpu.make_async_remote_copy(src_ref=src, dst_ref=dst, send_sem=send.at[idx], recv_sem=recv.at[idx],
                                          device_id={"row": row, "col": col}, device_id_type=MESH)
        cp.start()
        sent.append(cp)

    def got(idx, dst):
        pltpu.make_async_remote_copy(src_ref=dst, dst_ref=dst, send_sem=send.at[idx], recv_sem=recv.at[idx],
                                     device_id={"row": r, "col": c}, device_id_type=MESH).wait_recv()

    put(0, a_sd, sd_ref.at[c, r], yp, c)
    put(1, a_sd, sd_ref.at[c, r], ym, c)
    if wide:
        put(4, a_rp, rp_ref.at[c], r, xp)
        put(5, a_rp, rp_ref.at[c], r, xm)
        put(6, a_rp, rp_ref.at[c], r, par)
        put(13, a_up, up_ref.at[r], yp, c)
        put(14, a_up, up_ref.at[r], ym, c)
    sd_in.wait()
    sd_out = pltpu.make_async_copy(own_sd, sd_ref.at[c, r], loc.at[0])
    sd_out.start()
    if wide:
        rp_in.wait()
        rp_out = pltpu.make_async_copy(own_rp, rp_ref.at[c], loc.at[1])
        rp_out.start()
        up_in.wait()
        up_out = pltpu.make_async_copy(own_up, up_ref.at[r], loc.at[2])
        up_out.start()
    half_y = h // 2
    lo_y, hi_y = pl.ds(0, half_y), pl.ds(half_y, half_y)
    got(0, sd_ref.at[c, ym])
    put(2, sd_ref.at[c, ym, lo_y], sd_ref.at[c, ym, lo_y], yp, c)
    got(1, sd_ref.at[c, yp])
    put(3, sd_ref.at[c, yp, hi_y], sd_ref.at[c, yp, hi_y], ym, c)
    sd_out.wait()
    got(2, sd_ref.at[c, y2, lo_y])
    got(3, sd_ref.at[c, y2, hi_y])
    put(17, sd_ref.at[c], sd_ref.at[c], r, xp)
    put(18, sd_ref.at[c], sd_ref.at[c], r, xm)
    put(19, sd_ref.at[c], sd_ref.at[c], r, par)

    def ring_x_rest(first, ref, lo, hi):
        got(first, ref.at[xm])
        put(first + 3, ref.at[xm].at[lo], ref.at[xm].at[lo], r, xp)
        put(first + 5, ref.at[xm], ref.at[xm], r, par)
        got(first + 1, ref.at[xp])
        put(first + 4, ref.at[xp].at[hi], ref.at[xp].at[hi], r, xm)
        put(first + 6, ref.at[xp], ref.at[xp], r, par)

    def ring_x_end(first, ref, lo, hi):
        got(first + 3, ref.at[x2].at[lo])
        put(first + 7, ref.at[x2].at[lo], ref.at[x2].at[lo], r, par)
        got(first + 4, ref.at[x2].at[hi])
        put(first + 8, ref.at[x2].at[hi], ref.at[x2].at[hi], r, par)

    def ring_x_partner(first, ref, lo, hi):
        got(first + 2, ref.at[par])
        got(first + 5, ref.at[pxm])
        got(first + 6, ref.at[pxp])
        got(first + 7, ref.at[px2].at[lo])
        got(first + 8, ref.at[px2].at[hi])

    half_r = row_devs // 2
    sd_halves = (pl.ds(0, half_r), pl.ds(half_r, half_r))
    if wide:
        half_p = nr * blk // 2
        rp_halves = (pl.ds(0, half_p), pl.ds(half_p, half_p))
        ring_x_rest(4, rp_ref, *rp_halves)
        got(13, up_ref.at[ym])
        put(15, up_ref.at[ym, lo_y], up_ref.at[ym, lo_y], yp, c)
        got(14, up_ref.at[yp])
        put(16, up_ref.at[yp, hi_y], up_ref.at[yp, hi_y], ym, c)
    ring_x_rest(17, sd_ref, *sd_halves)
    if wide:
        ring_x_end(4, rp_ref, *rp_halves)
    ring_x_end(17, sd_ref, *sd_halves)
    if wide:
        got(15, up_ref.at[y2, lo_y])
        got(16, up_ref.at[y2, hi_y])
        ring_x_partner(4, rp_ref, *rp_halves)
        rp_out.wait()
        up_out.wait()
    ring_x_partner(17, sd_ref, *sd_halves)
    for cp in sent:
        cp.wait_send()


def gather(a2, s, blk, row_devs, col_devs, nr, nc):
    per = col_devs // row_devs
    h = per * blk
    outs = [jax.ShapeDtypeStruct((col_devs, row_devs, h, blk), F32)]
    scratch = [pltpu.VMEM((h, blk), F32)]
    if nc:
        outs += [jax.ShapeDtypeStruct((col_devs, nr * blk, blk), F32), jax.ShapeDtypeStruct((row_devs, h, nc * blk), F32)]
        scratch += [pltpu.VMEM((nr * blk, blk), F32), pltpu.VMEM((h, nc * blk), F32)]
    anyspec = pl.BlockSpec(memory_space=pl.ANY)
    return pl.pallas_call(
        functools.partial(gather_kernel, (s, blk, row_devs, col_devs, nr, nc)),
        out_shape=outs,
        in_specs=[anyspec],
        out_specs=[anyspec] * len(outs),
        scratch_shapes=scratch + [pltpu.SemaphoreType.DMA((26,)), pltpu.SemaphoreType.DMA((26,)), pltpu.SemaphoreType.DMA((3,))],
        compiler_params=pltpu.CompilerParams(collective_id=s, has_side_effects=True),
        name=f"gather_{s}",
    )(a2)


def last_kernel(dims, a_ref, sd_hbm, out_ref, sd, dblk, linv, bsd, whole, sdsem, loc):
    s, blk, row_devs, col_devs = dims
    h = (col_devs // row_devs) * blk
    r = lax.axis_index("row")
    c = lax.axis_index("col")
    sd_in = [pltpu.make_async_copy(sd_hbm.at[k], sd.at[k], sdsem.at[k]) for k in range(col_devs)]
    for cp in sd_in:
        cp.start()
    a_in = pltpu.make_async_copy(a_ref, whole, loc.at[0])
    a_in.start()
    a_out = pltpu.make_async_copy(whole, out_ref, loc.at[1])

    def at(j, k):
        return (k, j % row_devs, pl.ds((j // row_devs) * blk, blk))

    sd_in[0].wait()
    dblk[...] = sd[at(0, 0)]

    @pl.loop(0, col_devs)
    def _(k):
        lfac, inv = chol_inv(dblk[...])
        dblk[...] = lfac
        linv[k] = inv_operands(inv)
        for kk in range(col_devs):
            @pl.when(k == kk)
            def _():
                chain_rest(kk, at, sd_in, sd, dblk, linv, bsd, blk, col_devs)
                if kk == col_devs // 2:
                    a_in.wait()
                    a_out.start()

    for tt in range(col_devs // row_devs):
        val = sd[c, r, pl.ds(tt * blk, blk)]
        sd[c, r, pl.ds(tt * blk, blk)] = jnp.where(tt * row_devs + r >= c, val, jnp.zeros_like(val))
    a_out.wait()
    d_out = pltpu.make_async_copy(sd.at[c, r], out_ref.at[s, :, pl.ds(s * blk, blk)], loc.at[0])
    d_out.start()
    d_out.wait()


def last(a3, sd, s, blk, row_devs, col_devs):
    anyspec = pl.BlockSpec(memory_space=pl.ANY)
    h = (col_devs // row_devs) * blk
    return pl.pallas_call(
        functools.partial(last_kernel, (s, blk, row_devs, col_devs)),
        out_shape=jax.ShapeDtypeStruct(a3.shape, F32),
        in_specs=[anyspec, anyspec],
        out_specs=anyspec,
        scratch_shapes=[
            pltpu.VMEM((col_devs, row_devs, h, blk), F32),
            pltpu.VMEM((blk, blk), F32),
            pltpu.VMEM((col_devs, 3 * blk, 2 * blk), BF16),
            pltpu.VMEM((col_devs * blk, col_devs * blk), BF16),
            pltpu.VMEM(a3.shape, F32),
            pltpu.SemaphoreType.DMA((col_devs,)),
            pltpu.SemaphoreType.DMA((2,)),
        ],
        compiler_params=pltpu.CompilerParams(vmem_limit_bytes=60 * 1024 * 1024),
        name=f"last_{s}",
    )(a3, sd)


def chain_rest(kk, at, sd_in, sd, dblk, linv, bsd, blk, col_devs):
    sd[at(kk, kk)] = dblk[...]
    if kk + 1 < col_devs:
        sd_in[kk + 1].wait()
        below = jnp.concatenate([sd[at(j, kk)] for j in range(kk + 1, col_devs)], axis=0)
        low = solve_f32(below, linv[kk])
        for j in range(kk + 1, col_devs):
            sd[at(j, kk)] = low[(j - kk - 1) * blk:(j - kk) * blk]
        bsd[(kk + 1) * blk:, kk * blk:(kk + 1) * blk] = low.astype(BF16)
        upd = lax.dot_general(bsd[(kk + 1) * blk:, :(kk + 1) * blk], bsd[(kk + 1) * blk:(kk + 2) * blk, :(kk + 1) * blk], NT,
                              preferred_element_type=F32)
        dblk[...] = sd[at(kk + 1, kk + 1)] - upd[:blk]
        for j in range(kk + 2, col_devs):
            sd[at(j, kk + 1)] = sd[at(j, kk + 1)] - upd[(j - kk - 1) * blk:(j - kk) * blk]


def fused_kernel(dims, a_ref, sd_hbm, out_ref, sdn, sd, dblk, linv, bsd, zero, pan, up, w, bi, bj, bq, own, send, recv, loc, sdsem):
    s, blk, row_devs, col_devs, nq = dims
    h = (col_devs // row_devs) * blk
    r = lax.axis_index("row")
    c = lax.axis_index("col")
    cores = 2
    ring = col_devs // cores
    x, core = c // cores, c % cores
    yp, ym, y2 = (r + 1) % row_devs, (r + row_devs - 1) % row_devs, (r + 2) % row_devs
    ix = lambda d, k: ((x + d) % ring) * cores + k
    xp, xm, x2, par = ix(1, core), ix(ring - 1, core), ix(2, core), ix(0, 1 - core)
    pxp, pxm, px2 = ix(1, 1 - core), ix(ring - 1, 1 - core), ix(2, 1 - core)
    lanes = pl.ds(s * blk, blk)
    right = pl.ds((s + 1) * blk, nq * blk)
    under = pl.ds(s + 1, nq)
    a_rp, a_up = a_ref.at[under, :, lanes], a_ref.at[s, :, right]
    top, bot, both = pl.ds(0, blk), pl.ds(blk, blk), pl.ds(0, h)
    half = row_devs // 2
    lo, hi = pl.ds(0, half), pl.ds(half, half)
    table = {}

    def add(name, src, dst, row, col, arrive):
        table[name] = (len(table), src, dst, row, col, arrive)

    add("up+", a_up, up.at[r], yp, c, up.at[ym])
    add("up-", a_up, up.at[r], ym, c, up.at[yp])
    add("upf+", up.at[ym, top], up.at[ym, top], yp, c, up.at[y2, top])
    add("upf-", up.at[yp, bot], up.at[yp, bot], ym, c, up.at[y2, bot])
    rows = lambda i, part: pan.at[i, :, part]
    add("rp+", a_rp, rows(c, both), r, xp, rows(xm, both))
    add("rp-", a_rp, rows(c, both), r, xm, rows(xp, both))
    add("rpp", a_rp, rows(c, both), r, par, rows(par, both))
    add("rpf+", rows(xm, top), rows(xm, top), r, xp, rows(x2, top))
    add("rpf-", rows(xp, bot), rows(xp, bot), r, xm, rows(x2, bot))
    add("rpr1", rows(xm, both), rows(xm, both), r, par, rows(pxm, both))
    add("rpr2", rows(xp, both), rows(xp, both), r, par, rows(pxp, both))
    add("rpr3", rows(x2, top), rows(x2, top), r, par, rows(px2, top))
    add("rpr4", rows(x2, bot), rows(x2, bot), r, par, rows(px2, bot))
    add("sy+", sdn.at[c, r], sdn.at[c, r], yp, c, sdn.at[c, ym])
    add("sy-", sdn.at[c, r], sdn.at[c, r], ym, c, sdn.at[c, yp])
    add("syf+", sdn.at[c, ym, top], sdn.at[c, ym, top], yp, c, sdn.at[c, y2, top])
    add("syf-", sdn.at[c, yp, bot], sdn.at[c, yp, bot], ym, c, sdn.at[c, y2, bot])
    for tag, part in (("lo", lo), ("hi", hi)):
        add("sx+" + tag, sdn.at[c, part], sdn.at[c, part], r, xp, sdn.at[xm, part])
        add("sx-" + tag, sdn.at[c, part], sdn.at[c, part], r, xm, sdn.at[xp, part])
        add("sr1" + tag, sdn.at[xm, part], sdn.at[xm, part], r, par, sdn.at[pxm, part])
        add("sr2" + tag, sdn.at[xp, part], sdn.at[xp, part], r, par, sdn.at[pxp, part])
        add("sr3" + tag, sdn.at[x2, part], sdn.at[x2, part], r, par, sdn.at[px2, part])
    add("sxp", sdn.at[c], sdn.at[c], r, par, sdn.at[par])
    add("sxf+", sdn.at[xm, lo], sdn.at[xm, lo], r, xp, sdn.at[x2, lo])
    add("sxf-", sdn.at[xp, hi], sdn.at[xp, hi], r, xm, sdn.at[x2, hi])

    def remote(name):
        idx, src, dst, row, col, _ = table[name]
        return pltpu.make_async_remote_copy(src_ref=src, dst_ref=dst, send_sem=send.at[idx], recv_sem=recv.at[idx],
                                            device_id={"row": row, "col": col}, device_id_type=MESH)

    def start(*names):
        for name in names:
            remote(name).start()

    def got(*names):
        for name in names:
            idx, arrive = table[name][0], table[name][5]
            pltpu.make_async_remote_copy(src_ref=arrive, dst_ref=arrive, send_sem=send.at[idx], recv_sem=recv.at[idx],
                                         device_id={"row": r, "col": c}, device_id_type=MESH).wait_recv()

    def gone(*names):
        for name in names:
            remote(name).wait_send()

    sd_in = [pltpu.make_async_copy(sd_hbm.at[k], sd.at[k], sdsem.at[k]) for k in range(col_devs)]
    for cp in sd_in:
        cp.start()
    rp_in = pltpu.make_async_copy(a_rp, rows(c, both), loc.at[0])
    up_in = pltpu.make_async_copy(a_up, up.at[r], loc.at[1])
    w_in = pltpu.make_async_copy(a_ref.at[under, :, right], w, loc.at[2])
    z_out = pltpu.make_async_copy(zero, out_ref.at[s, :, right], loc.at[3])
    d_out = pltpu.make_async_copy(sd.at[c, r], out_ref.at[s, :, lanes], loc.at[4])
    l_out = pltpu.make_async_copy(rows(c, both), out_ref.at[under, :, lanes], loc.at[5])
    n_out = pltpu.make_async_copy(own, sdn.at[c, r], loc.at[6])
    w_out = pltpu.make_async_copy(w, out_ref.at[under, :, right], loc.at[7])

    barrier = pltpu.get_barrier_semaphore()
    for row, col in ((yp, c), (ym, c), (r, xp), (r, xm), (r, par)):
        pl.semaphore_signal(barrier, inc=1, device_id={"row": row, "col": col}, device_id_type=MESH)
    pl.semaphore_wait(barrier, 5)
    start("rp+", "rp-", "up+", "up-", "rpp")
    rp_in.start()
    up_in.start()
    w_in.start()
    zero[...] = jnp.zeros_like(zero)

    def at(j, k):
        return (k, j % row_devs, pl.ds((j // row_devs) * blk, blk))

    fwd_k = min(col_devs - 2, -(-9 * nq // 14))
    end_k = min(col_devs - 1, nq + 1)
    sd_in[0].wait()
    dblk[...] = sd[at(0, 0)]

    @pl.loop(0, col_devs)
    def _(k):
        lfac, inv = chol_inv(dblk[...])
        dblk[...] = lfac
        linv[k] = inv_operands(inv)
        for kk in range(col_devs):
            @pl.when(k == kk)
            def _():
                chain_rest(kk, at, sd_in, sd, dblk, linv, bsd, blk, col_devs)
                if kk == fwd_k:
                    got("rp+")
                    start("rpf+", "rpr1")
                    got("rp-")
                    start("rpf-", "rpr2")
                    got("up+")
                    start("upf+")
                    got("up-")
                    start("upf-")
                if kk == end_k:
                    got("rpf+")
                    start("rpr3")
                    got("rpf-")
                    start("rpr4")

    for tt in range(col_devs // row_devs):
        val = sd[c, r, pl.ds(tt * blk, blk)]
        sd[c, r, pl.ds(tt * blk, blk)] = jnp.where(tt * row_devs + r >= c, val, jnp.zeros_like(val))
    d_out.start()
    up_in.wait()
    gone("up+", "up-")
    z_out.start()
    rp_in.wait()
    got("rpp", "rpr1", "rpr2", "rpr3", "rpr4", "upf+", "upf-")
    gone("rp+", "rp-", "rpp", "rpf+", "rpf-", "rpr1", "rpr2", "rpr3", "rpr4", "upf+", "upf-")
    w_in.wait()

    def stage_a():
        got("sy+")
        start("syf+")
        got("sy-")
        start("syf-")

    def stage_b():
        got("syf+", "syf-")
        start("sx+lo", "sx-hi", "sx+hi", "sx-lo", "sxp")

    def stage_c():
        got("sx+lo")
        start("sxf+", "sr1lo")
        got("sx-hi")
        start("sxf-", "sr2hi")

    def stage_d():
        got("sx+hi")
        start("sr1hi")
        got("sx-lo")
        start("sr2lo")

    def stage_e():
        got("sxf+")
        start("sr3lo")
        got("sxf-")
        start("sr3hi")

    stages = [(2, stage_a), (3, stage_b), (5, stage_c), (7, stage_d), (10, stage_e)]

    @pl.loop(0, nq)
    def _(q):
        for k in range(col_devs):
            ops = linv[k]
            pan[k, q, pl.ds(h, blk)] = up[k % row_devs, pl.ds((k // row_devs) * blk, blk), pl.ds(pl.multiple_of(q * blk, blk), blk)].T
            cur = pan[k, q]
            if k:
                cur = cur - lax.dot_general(bq[:, :k * blk], bsd[k * blk:(k + 1) * blk, :k * blk], NT, preferred_element_type=F32)
            low = solve_f32(cur, ops)
            pan[k, q] = low
            bq[:, k * blk:(k + 1) * blk] = low.astype(BF16)
        bi[q] = bq[:h]
        bj[pl.ds(pl.multiple_of(q * blk, blk), blk)] = bq[h:]

        @pl.when(q == 0)
        def _():
            own[...] = w[0, :, :blk] - lax.dot_general(bq[:h], bq[h:], NT, preferred_element_type=F32)
            n_out.start()
            n_out.wait()
            start("sy+", "sy-")
        for pos, fn in stages:
            if pos < nq:
                pl.when(q == pos)(fn)

    l_out.start()

    @pl.loop(0, nq)
    def _(q):
        w[q] = w[q] - lax.dot_general(bi[q], bj[...], NT, preferred_element_type=F32)
        for pos, fn in stages:
            if nq <= pos < 2 * nq:
                pl.when(q == pos - nq)(fn)

    w_out.start()
    for pos, fn in stages:
        if pos >= 2 * nq:
            fn()
    l_out.wait()
    z_out.wait()
    d_out.wait()
    got("sxp", "sr1lo", "sr1hi", "sr2lo", "sr2hi", "sr3lo", "sr3hi")
    gone("sy+", "sy-", "syf+", "syf-", "sx+lo", "sx+hi", "sx-lo", "sx-hi", "sxp", "sxf+", "sxf-",
         "sr1lo", "sr1hi", "sr2lo", "sr2hi", "sr3lo", "sr3hi")
    w_out.wait()


def fused(a3, sd, s, blk, row_devs, col_devs, nq):
    h = (col_devs // row_devs) * blk
    anyspec = pl.BlockSpec(memory_space=pl.ANY)
    scratch = [
        pltpu.VMEM((col_devs, row_devs, h, blk), F32),
        pltpu.VMEM((blk, blk), F32),
        pltpu.VMEM((col_devs, 3 * blk, 2 * blk), BF16),
        pltpu.VMEM((col_devs * blk, col_devs * blk), BF16),
        pltpu.VMEM((h, nq * blk), F32),
        pltpu.VMEM((col_devs, nq, h + blk, blk), F32),
        pltpu.VMEM((row_devs, h, nq * blk), F32),
        pltpu.VMEM((nq, h, nq * blk), F32),
        pltpu.VMEM((nq, h, col_devs * blk), BF16),
        pltpu.VMEM((nq * blk, col_devs * blk), BF16),
        pltpu.VMEM((h + blk, col_devs * blk), BF16),
        pltpu.VMEM((h, blk), F32),
        pltpu.SemaphoreType.DMA((32,)),
        pltpu.SemaphoreType.DMA((32,)),
        pltpu.SemaphoreType.DMA((8,)),
        pltpu.SemaphoreType.DMA((col_devs,)),
    ]
    return pl.pallas_call(
        functools.partial(fused_kernel, (s, blk, row_devs, col_devs, nq)),
        out_shape=[jax.ShapeDtypeStruct(a3.shape, F32), jax.ShapeDtypeStruct(sd.shape, F32)],
        in_specs=[anyspec, anyspec],
        out_specs=[anyspec, anyspec],
        scratch_shapes=scratch,
        input_output_aliases={} if s == 0 else {0: 0},
        compiler_params=pltpu.CompilerParams(vmem_limit_bytes=60 * 1024 * 1024, collective_id=s + 1, has_side_effects=True),
        name=f"fused_{s}",
    )(a3, sd)


def solution(mesh):
    row_devs = mesh.shape["row"]
    col_devs = mesh.shape["col"]
    per = col_devs // row_devs

    def factor_local(a_loc):
        row_blocks, blk, local_cols = a_loc.shape
        steps = local_cols // blk
        (sd,) = gather(a_loc.reshape(row_blocks * blk, local_cols), 0, blk, row_devs, col_devs, 0, 0)
        a3 = a_loc.reshape(steps, per * blk, local_cols)
        for s in range(steps - 1):
            a3, sd = fused(a3, sd, s, blk, row_devs, col_devs, steps - 1 - s)
        a3 = last(a3, sd, steps - 1, blk, row_devs, col_devs)
        return a3.reshape(row_blocks, blk, local_cols)

    spec = P(("batch", "row"), None, "col")
    return jax.shard_map(factor_local, mesh=mesh, in_specs=(spec,), out_specs=spec, check_vma=False)
```

```python
import functools
import jax
import jax.numpy as jnp
from jax import lax
from jax.experimental import pallas as pl
from jax.experimental.pallas import tpu as pltpu
from jax.sharding import PartitionSpec as P

MESH = pl.DeviceIdType.MESH
F32 = jnp.float32
BF16 = jnp.bfloat16
SUB = 8
NT = (((1,), (1,)), ((), ()))


def chol_inv(blk):
    n = blk.shape[0]
    groups = n // SUB
    lane = lax.broadcasted_iota(jnp.int32, (SUB, n), 1)
    sub = lax.broadcasted_iota(jnp.int32, (SUB, n), 0)
    ident = lane - sub
    spread = lambda v: jnp.broadcast_to(v, (SUB, n))
    pull = lambda rows, at: jnp.concatenate([spread(rows[:, at + m:at + m + 1])[None] for m in range(SUB)], axis=0)
    t0, t1, rest = blk[:SUB], blk[SUB:2 * SUB], blk[2 * SUB:]
    upper, diag, inv_rows = [], [], []
    c0, c1 = pull(t0, 0), pull(t1, 0)
    for p in range(groups):
        base = p * SUB
        inside = (lane >= base) & (lane < base + SUB)
        t0 = jnp.where(inside, jnp.where(ident == base, 1.0, 0.0), t0)
        if t1 is not None:
            t1 = jnp.where(inside, 0.0, t1)
        if rest is not None:
            wide = jnp.concatenate([inside] * (rest.shape[0] // SUB), axis=0)
            rest = jnp.where(wide, 0.0, rest)
        o = jnp.zeros((SUB, n), F32)
        urows = []
        for j in range(SUB):
            r = lax.rsqrt(spread(c0[j, j:j + 1]))
            l0 = c0[j] * r
            l0m = jnp.where(sub > j, l0, 0.0)
            urow = spread(t0[j:j + 1]) * r
            urows.append(urow)
            t0 = jnp.where(sub == j, urow, t0 - l0m * urow)
            o = jnp.where((lane == base + j) & (sub >= j), l0, o)
            if j + 1 < SUB:
                spl = jnp.broadcast_to(c0[j + 1:, j:j + 1], (SUB - 1 - j, SUB, n)) * r[None]
                c0 = jnp.concatenate([c0[:j + 1], c0[j + 1:] - l0m[None] * spl], axis=0)
            if t1 is not None:
                l1 = c1[j] * r
                t1 = t1 - l1 * urow
                if j + 1 < SUB:
                    c1 = jnp.concatenate([c1[:j + 1], c1[j + 1:] - l1[None] * spl], axis=0)
        inv_rows.append(jnp.where(lane < base + SUB, t0, 0.0))
        upper.append(jnp.where(lane >= base + SUB, t0, 0.0))
        diag.append(o)
        if t1 is None:
            break
        c0 = pull(t1, base + SUB)
        nxt = None
        if rest is not None:
            ut = t0.T[base + 2 * SUB:]
            nxt, more = rest[:SUB], rest[SUB:]
            for j in range(SUB):
                nxt = nxt - spread(ut[:SUB, j:j + 1]) * urows[j]
            c1 = pull(nxt, base + SUB)
            rest = None
            if more.shape[0]:
                for j in range(SUB):
                    tall = jnp.concatenate([urows[j]] * (more.shape[0] // SUB), axis=0)
                    more = more - jnp.broadcast_to(ut[SUB:, j:j + 1], more.shape) * tall
                rest = more
        t0, t1 = t1, nxt
    lfac = jnp.concatenate(upper, axis=0).T + jnp.concatenate(diag, axis=0)
    return lfac, jnp.concatenate(inv_rows, axis=0)


def split3(x):
    hi = x.astype(BF16)
    rest = x - hi.astype(F32)
    mid = rest.astype(BF16)
    lo = (rest - mid.astype(F32)).astype(BF16)
    return hi, mid, lo


def inv_operands(linv):
    w1, w2, w3 = split3(linv)
    top = jnp.concatenate([w2, w1], axis=1)
    bot = jnp.concatenate([w1, w2], axis=1)
    return jnp.concatenate([top, bot, jnp.concatenate([w3, w1], axis=1)], axis=0)


def solve_f32(x, ops):
    n = x.shape[1]
    x1, x2, x3 = split3(x)
    main = lax.dot_general(jnp.concatenate([x1, x2], axis=1), ops[:2 * n], NT, preferred_element_type=F32)
    tail = lax.dot_general(jnp.concatenate([x1, x3], axis=1), ops[2 * n:], NT, preferred_element_type=F32)
    return (tail + main[:, :n]) + main[:, n:]


def gather_kernel(dims, a_ref, sd_ref, *rest):
    s, blk, row_devs, col_devs, nr, nc = dims
    wide = nc > 0
    if wide:
        rp_ref, up_ref, own_sd, own_rp, own_up, send, recv, loc = rest
    else:
        own_sd, send, recv, loc = rest
    per = col_devs // row_devs
    r = lax.axis_index("row")
    c = lax.axis_index("col")
    cores = 2
    ring_x = col_devs // cores
    x, core = c // cores, c % cores
    yp, ym, y2 = (r + 1) % row_devs, (r + row_devs - 1) % row_devs, (r + 2) % row_devs
    xp = ((x + 1) % ring_x) * cores + core
    xm = ((x + ring_x - 1) % ring_x) * cores + core
    x2 = ((x + 2) % ring_x) * cores + core
    par = x * cores + (1 - core)
    pxp, pxm, px2 = ((x + 1) % ring_x) * cores + 1 - core, ((x + ring_x - 1) % ring_x) * cores + 1 - core, ((x + 2) % ring_x) * cores + 1 - core

    h = per * blk
    row0, col0 = s * h, s * blk
    a_sd = a_ref.at[pl.ds(row0, h), pl.ds(col0, blk)]
    sd_in = pltpu.make_async_copy(a_sd, own_sd, loc.at[0])
    sd_in.start()
    if wide:
        a_rp = a_ref.at[pl.ds(row0 + h, nr * blk), pl.ds(col0, blk)]
        a_up = a_ref.at[pl.ds(row0, h), pl.ds(col0 + blk, nc * blk)]
        rp_in = pltpu.make_async_copy(a_rp, own_rp, loc.at[1])
        up_in = pltpu.make_async_copy(a_up, own_up, loc.at[2])
        rp_in.start()
        up_in.start()

    barrier = pltpu.get_barrier_semaphore()
    for row, col in ((yp, c), (ym, c), (r, xp), (r, xm), (r, par)):
        pl.semaphore_signal(barrier, inc=1, device_id={"row": row, "col": col}, device_id_type=MESH)
    pl.semaphore_wait(barrier, 5)

    sent = []

    def put(idx, src, dst, row, col):
        cp = pltpu.make_async_remote_copy(src_ref=src, dst_ref=dst, send_sem=send.at[idx], recv_sem=recv.at[idx],
                                          device_id={"row": row, "col": col}, device_id_type=MESH)
        cp.start()
        sent.append(cp)

    def got(idx, dst):
        pltpu.make_async_remote_copy(src_ref=dst, dst_ref=dst, send_sem=send.at[idx], recv_sem=recv.at[idx],
                                     device_id={"row": r, "col": c}, device_id_type=MESH).wait_recv()

    put(0, a_sd, sd_ref.at[c, r], yp, c)
    put(1, a_sd, sd_ref.at[c, r], ym, c)
    if wide:
        put(4, a_rp, rp_ref.at[c], r, xp)
        put(5, a_rp, rp_ref.at[c], r, xm)
        put(6, a_rp, rp_ref.at[c], r, par)
        put(13, a_up, up_ref.at[r], yp, c)
        put(14, a_up, up_ref.at[r], ym, c)
    sd_in.wait()
    sd_out = pltpu.make_async_copy(own_sd, sd_ref.at[c, r], loc.at[0])
    sd_out.start()
    if wide:
        rp_in.wait()
        rp_out = pltpu.make_async_copy(own_rp, rp_ref.at[c], loc.at[1])
        rp_out.start()
        up_in.wait()
        up_out = pltpu.make_async_copy(own_up, up_ref.at[r], loc.at[2])
        up_out.start()
    half_y = h // 2
    lo_y, hi_y = pl.ds(0, half_y), pl.ds(half_y, half_y)
    got(0, sd_ref.at[c, ym])
    put(2, sd_ref.at[c, ym, lo_y], sd_ref.at[c, ym, lo_y], yp, c)
    got(1, sd_ref.at[c, yp])
    put(3, sd_ref.at[c, yp, hi_y], sd_ref.at[c, yp, hi_y], ym, c)
    sd_out.wait()
    got(2, sd_ref.at[c, y2, lo_y])
    got(3, sd_ref.at[c, y2, hi_y])
    put(17, sd_ref.at[c], sd_ref.at[c], r, xp)
    put(18, sd_ref.at[c], sd_ref.at[c], r, xm)
    put(19, sd_ref.at[c], sd_ref.at[c], r, par)

    def ring_x_rest(first, ref, lo, hi):
        got(first, ref.at[xm])
        put(first + 3, ref.at[xm].at[lo], ref.at[xm].at[lo], r, xp)
        put(first + 5, ref.at[xm], ref.at[xm], r, par)
        got(first + 1, ref.at[xp])
        put(first + 4, ref.at[xp].at[hi], ref.at[xp].at[hi], r, xm)
        put(first + 6, ref.at[xp], ref.at[xp], r, par)

    def ring_x_end(first, ref, lo, hi):
        got(first + 3, ref.at[x2].at[lo])
        put(first + 7, ref.at[x2].at[lo], ref.at[x2].at[lo], r, par)
        got(first + 4, ref.at[x2].at[hi])
        put(first + 8, ref.at[x2].at[hi], ref.at[x2].at[hi], r, par)

    def ring_x_partner(first, ref, lo, hi):
        got(first + 2, ref.at[par])
        got(first + 5, ref.at[pxm])
        got(first + 6, ref.at[pxp])
        got(first + 7, ref.at[px2].at[lo])
        got(first + 8, ref.at[px2].at[hi])

    half_r = row_devs // 2
    sd_halves = (pl.ds(0, half_r), pl.ds(half_r, half_r))
    if wide:
        half_p = nr * blk // 2
        rp_halves = (pl.ds(0, half_p), pl.ds(half_p, half_p))
        ring_x_rest(4, rp_ref, *rp_halves)
        got(13, up_ref.at[ym])
        put(15, up_ref.at[ym, lo_y], up_ref.at[ym, lo_y], yp, c)
        got(14, up_ref.at[yp])
        put(16, up_ref.at[yp, hi_y], up_ref.at[yp, hi_y], ym, c)
    ring_x_rest(17, sd_ref, *sd_halves)
    if wide:
        ring_x_end(4, rp_ref, *rp_halves)
    ring_x_end(17, sd_ref, *sd_halves)
    if wide:
        got(15, up_ref.at[y2, lo_y])
        got(16, up_ref.at[y2, hi_y])
        ring_x_partner(4, rp_ref, *rp_halves)
        rp_out.wait()
        up_out.wait()
    ring_x_partner(17, sd_ref, *sd_halves)
    for cp in sent:
        cp.wait_send()


def gather(a2, s, blk, row_devs, col_devs, nr, nc):
    per = col_devs // row_devs
    h = per * blk
    outs = [jax.ShapeDtypeStruct((col_devs, row_devs, h, blk), F32)]
    scratch = [pltpu.VMEM((h, blk), F32)]
    if nc:
        outs += [jax.ShapeDtypeStruct((col_devs, nr * blk, blk), F32), jax.ShapeDtypeStruct((row_devs, h, nc * blk), F32)]
        scratch += [pltpu.VMEM((nr * blk, blk), F32), pltpu.VMEM((h, nc * blk), F32)]
    anyspec = pl.BlockSpec(memory_space=pl.ANY)
    return pl.pallas_call(
        functools.partial(gather_kernel, (s, blk, row_devs, col_devs, nr, nc)),
        out_shape=outs,
        in_specs=[anyspec],
        out_specs=[anyspec] * len(outs),
        scratch_shapes=scratch + [pltpu.SemaphoreType.DMA((26,)), pltpu.SemaphoreType.DMA((26,)), pltpu.SemaphoreType.DMA((3,))],
        compiler_params=pltpu.CompilerParams(collective_id=s, has_side_effects=True),
        name=f"gather_{s}",
    )(a2)


def last_kernel(dims, a_ref, sd_hbm, out_ref, sd, dblk, linv, bsd, whole, sdsem, loc):
    s, blk, row_devs, col_devs = dims
    h = (col_devs // row_devs) * blk
    r = lax.axis_index("row")
    c = lax.axis_index("col")
    sd_in = [pltpu.make_async_copy(sd_hbm.at[k], sd.at[k], sdsem.at[k]) for k in range(col_devs)]
    for cp in sd_in:
        cp.start()
    a_in = pltpu.make_async_copy(a_ref, whole, loc.at[0])
    a_in.start()
    a_out = pltpu.make_async_copy(whole, out_ref, loc.at[1])

    def at(j, k):
        return (k, j % row_devs, pl.ds((j // row_devs) * blk, blk))

    sd_in[0].wait()
    dblk[...] = sd[at(0, 0)]

    @pl.loop(0, col_devs)
    def _(k):
        lfac, inv = chol_inv(dblk[...])
        dblk[...] = lfac
        linv[k] = inv_operands(inv)
        for kk in range(col_devs):
            @pl.when(k == kk)
            def _():
                chain_rest(kk, at, sd_in, sd, dblk, linv, bsd, blk, col_devs)
                if kk == col_devs // 2:
                    a_in.wait()
                    a_out.start()

    for tt in range(col_devs // row_devs):
        val = sd[c, r, pl.ds(tt * blk, blk)]
        sd[c, r, pl.ds(tt * blk, blk)] = jnp.where(tt * row_devs + r >= c, val, jnp.zeros_like(val))
    a_out.wait()
    d_out = pltpu.make_async_copy(sd.at[c, r], out_ref.at[s, :, pl.ds(s * blk, blk)], loc.at[0])
    d_out.start()
    d_out.wait()


def last(a3, sd, s, blk, row_devs, col_devs):
    anyspec = pl.BlockSpec(memory_space=pl.ANY)
    h = (col_devs // row_devs) * blk
    return pl.pallas_call(
        functools.partial(last_kernel, (s, blk, row_devs, col_devs)),
        out_shape=jax.ShapeDtypeStruct(a3.shape, F32),
        in_specs=[anyspec, anyspec],
        out_specs=anyspec,
        scratch_shapes=[
            pltpu.VMEM((col_devs, row_devs, h, blk), F32),
            pltpu.VMEM((blk, blk), F32),
            pltpu.VMEM((col_devs, 3 * blk, 2 * blk), BF16),
            pltpu.VMEM((col_devs * blk, col_devs * blk), BF16),
            pltpu.VMEM(a3.shape, F32),
            pltpu.SemaphoreType.DMA((col_devs,)),
            pltpu.SemaphoreType.DMA((2,)),
        ],
        compiler_params=pltpu.CompilerParams(vmem_limit_bytes=60 * 1024 * 1024),
        name=f"last_{s}",
    )(a3, sd)


def chain_rest(kk, at, sd_in, sd, dblk, linv, bsd, blk, col_devs):
    sd[at(kk, kk)] = dblk[...]
    if kk + 1 < col_devs:
        sd_in[kk + 1].wait()
        below = jnp.concatenate([sd[at(j, kk)] for j in range(kk + 1, col_devs)], axis=0)
        low = solve_f32(below, linv[kk])
        for j in range(kk + 1, col_devs):
            sd[at(j, kk)] = low[(j - kk - 1) * blk:(j - kk) * blk]
        bsd[(kk + 1) * blk:, kk * blk:(kk + 1) * blk] = low.astype(BF16)
        upd = lax.dot_general(bsd[(kk + 1) * blk:, :(kk + 1) * blk], bsd[(kk + 1) * blk:(kk + 2) * blk, :(kk + 1) * blk], NT,
                              preferred_element_type=F32)
        dblk[...] = sd[at(kk + 1, kk + 1)] - upd[:blk]
        for j in range(kk + 2, col_devs):
            sd[at(j, kk + 1)] = sd[at(j, kk + 1)] - upd[(j - kk - 1) * blk:(j - kk) * blk]


def fused_kernel(dims, a_ref, sd_hbm, out_ref, sdn, sd, dblk, linv, bsd, zero, pan, up, w, bi, bj, bq, own, send, recv, loc, sdsem):
    s, blk, row_devs, col_devs, nq = dims
    h = (col_devs // row_devs) * blk
    r = lax.axis_index("row")
    c = lax.axis_index("col")
    cores = 2
    ring = col_devs // cores
    x, core = c // cores, c % cores
    yp, ym, y2 = (r + 1) % row_devs, (r + row_devs - 1) % row_devs, (r + 2) % row_devs
    ix = lambda d, k: ((x + d) % ring) * cores + k
    xp, xm, x2, par = ix(1, core), ix(ring - 1, core), ix(2, core), ix(0, 1 - core)
    pxp, pxm, px2 = ix(1, 1 - core), ix(ring - 1, 1 - core), ix(2, 1 - core)
    lanes = pl.ds(s * blk, blk)
    right = pl.ds((s + 1) * blk, nq * blk)
    under = pl.ds(s + 1, nq)
    a_rp, a_up = a_ref.at[under, :, lanes], a_ref.at[s, :, right]
    top, bot, both = pl.ds(0, blk), pl.ds(blk, blk), pl.ds(0, h)
    half = row_devs // 2
    lo, hi = pl.ds(0, half), pl.ds(half, half)
    table = {}

    def add(name, src, dst, row, col, arrive):
        table[name] = (len(table), src, dst, row, col, arrive)

    add("up+", a_up, up.at[r], yp, c, up.at[ym])
    add("up-", a_up, up.at[r], ym, c, up.at[yp])
    add("upf+", up.at[ym, top], up.at[ym, top], yp, c, up.at[y2, top])
    add("upf-", up.at[yp, bot], up.at[yp, bot], ym, c, up.at[y2, bot])
    rows = lambda i, part: pan.at[i, :, part]
    add("rp+", a_rp, rows(c, both), r, xp, rows(xm, both))
    add("rp-", a_rp, rows(c, both), r, xm, rows(xp, both))
    add("rpp", a_rp, rows(c, both), r, par, rows(par, both))
    add("rpf+", rows(xm, top), rows(xm, top), r, xp, rows(x2, top))
    add("rpf-", rows(xp, bot), rows(xp, bot), r, xm, rows(x2, bot))
    add("rpr1", rows(xm, both), rows(xm, both), r, par, rows(pxm, both))
    add("rpr2", rows(xp, both), rows(xp, both), r, par, rows(pxp, both))
    add("rpr3", rows(x2, top), rows(x2, top), r, par, rows(px2, top))
    add("rpr4", rows(x2, bot), rows(x2, bot), r, par, rows(px2, bot))
    add("sy+", sdn.at[c, r], sdn.at[c, r], yp, c, sdn.at[c, ym])
    add("sy-", sdn.at[c, r], sdn.at[c, r], ym, c, sdn.at[c, yp])
    add("syf+", sdn.at[c, ym, top], sdn.at[c, ym, top], yp, c, sdn.at[c, y2, top])
    add("syf-", sdn.at[c, yp, bot], sdn.at[c, yp, bot], ym, c, sdn.at[c, y2, bot])
    for tag, part in (("lo", lo), ("hi", hi)):
        add("sx+" + tag, sdn.at[c, part], sdn.at[c, part], r, xp, sdn.at[xm, part])
        add("sx-" + tag, sdn.at[c, part], sdn.at[c, part], r, xm, sdn.at[xp, part])
        add("sr1" + tag, sdn.at[xm, part], sdn.at[xm, part], r, par, sdn.at[pxm, part])
        add("sr2" + tag, sdn.at[xp, part], sdn.at[xp, part], r, par, sdn.at[pxp, part])
        add("sr3" + tag, sdn.at[x2, part], sdn.at[x2, part], r, par, sdn.at[px2, part])
    add("sxp", sdn.at[c], sdn.at[c], r, par, sdn.at[par])
    add("sxf+", sdn.at[xm, lo], sdn.at[xm, lo], r, xp, sdn.at[x2, lo])
    add("sxf-", sdn.at[xp, hi], sdn.at[xp, hi], r, xm, sdn.at[x2, hi])

    def remote(name):
        idx, src, dst, row, col, _ = table[name]
        return pltpu.make_async_remote_copy(src_ref=src, dst_ref=dst, send_sem=send.at[idx], recv_sem=recv.at[idx],
                                            device_id={"row": row, "col": col}, device_id_type=MESH)

    def start(*names):
        for name in names:
            remote(name).start()

    def got(*names):
        for name in names:
            idx, arrive = table[name][0], table[name][5]
            pltpu.make_async_remote_copy(src_ref=arrive, dst_ref=arrive, send_sem=send.at[idx], recv_sem=recv.at[idx],
                                         device_id={"row": r, "col": c}, device_id_type=MESH).wait_recv()

    def gone(*names):
        for name in names:
            remote(name).wait_send()

    sd_in = [pltpu.make_async_copy(sd_hbm.at[k], sd.at[k], sdsem.at[k]) for k in range(col_devs)]
    for cp in sd_in:
        cp.start()
    rp_in = pltpu.make_async_copy(a_rp, rows(c, both), loc.at[0])
    up_in = pltpu.make_async_copy(a_up, up.at[r], loc.at[1])
    w_in = pltpu.make_async_copy(a_ref.at[under, :, right], w, loc.at[2])
    z_out = pltpu.make_async_copy(zero, out_ref.at[s, :, right], loc.at[3])
    d_out = pltpu.make_async_copy(sd.at[c, r], out_ref.at[s, :, lanes], loc.at[4])
    l_out = pltpu.make_async_copy(rows(c, both), out_ref.at[under, :, lanes], loc.at[5])
    n_out = pltpu.make_async_copy(own, sdn.at[c, r], loc.at[6])
    w_out = pltpu.make_async_copy(w, out_ref.at[under, :, right], loc.at[7])

    barrier = pltpu.get_barrier_semaphore()
    for row, col in ((yp, c), (ym, c), (r, xp), (r, xm), (r, par)):
        pl.semaphore_signal(barrier, inc=1, device_id={"row": row, "col": col}, device_id_type=MESH)
    pl.semaphore_wait(barrier, 5)
    start("rp+", "rp-", "up+", "up-", "rpp")
    rp_in.start()
    up_in.start()
    w_in.start()
    zero[...] = jnp.zeros_like(zero)

    def at(j, k):
        return (k, j % row_devs, pl.ds((j // row_devs) * blk, blk))

    fwd_k = min(col_devs - 2, -(-9 * nq // 14))
    end_k = min(col_devs - 1, nq + 1)
    sd_in[0].wait()
    dblk[...] = sd[at(0, 0)]

    @pl.loop(0, col_devs)
    def _(k):
        lfac, inv = chol_inv(dblk[...])
        dblk[...] = lfac
        linv[k] = inv_operands(inv)
        for kk in range(col_devs):
            @pl.when(k == kk)
            def _():
                chain_rest(kk, at, sd_in, sd, dblk, linv, bsd, blk, col_devs)
                if kk == fwd_k:
                    got("rp+")
                    start("rpf+", "rpr1")
                    got("rp-")
                    start("rpf-", "rpr2")
                    got("up+")
                    start("upf+")
                    got("up-")
                    start("upf-")
                if kk == end_k:
                    got("rpf+")
                    start("rpr3")
                    got("rpf-")
                    start("rpr4")

    for tt in range(col_devs // row_devs):
        val = sd[c, r, pl.ds(tt * blk, blk)]
        sd[c, r, pl.ds(tt * blk, blk)] = jnp.where(tt * row_devs + r >= c, val, jnp.zeros_like(val))
    d_out.start()
    up_in.wait()
    gone("up+", "up-")
    z_out.start()
    rp_in.wait()
    got("rpp", "rpr1", "rpr2", "rpr3", "rpr4", "upf+", "upf-")
    gone("rp+", "rp-", "rpp", "rpf+", "rpf-", "rpr1", "rpr2", "rpr3", "rpr4", "upf+", "upf-")
    w_in.wait()

    def stage_a():
        got("sy+")
        start("syf+")
        got("sy-")
        start("syf-")

    def stage_b():
        got("syf+", "syf-")
        start("sx+lo", "sx-hi", "sx+hi", "sx-lo", "sxp")

    def stage_c():
        got("sx+lo")
        start("sxf+", "sr1lo")
        got("sx-hi")
        start("sxf-", "sr2hi")

    def stage_d():
        got("sx+hi")
        start("sr1hi")
        got("sx-lo")
        start("sr2lo")

    def stage_e():
        got("sxf+")
        start("sr3lo")
        got("sxf-")
        start("sr3hi")

    stages = [(2, stage_a), (3, stage_b), (5, stage_c), (7, stage_d), (10, stage_e)]

    @pl.loop(0, nq)
    def _(q):
        for k in range(col_devs):
            ops = linv[k]
            pan[k, q, pl.ds(h, blk)] = up[k % row_devs, pl.ds((k // row_devs) * blk, blk), pl.ds(pl.multiple_of(q * blk, blk), blk)].T
            cur = pan[k, q]
            if k:
                cur = cur - lax.dot_general(bq[:, :k * blk], bsd[k * blk:(k + 1) * blk, :k * blk], NT, preferred_element_type=F32)
            low = solve_f32(cur, ops)
            pan[k, q] = low
            bq[:, k * blk:(k + 1) * blk] = low.astype(BF16)
        bi[q] = bq[:h]
        bj[pl.ds(pl.multiple_of(q * blk, blk), blk)] = bq[h:]

        @pl.when(q == 0)
        def _():
            own[...] = w[0, :, :blk] - lax.dot_general(bq[:h], bq[h:], NT, preferred_element_type=F32)
            n_out.start()
            n_out.wait()
            start("sy+", "sy-")
        for pos, fn in stages:
            if pos < nq:
                pl.when(q == pos)(fn)

    l_out.start()

    @pl.loop(0, nq)
    def _(q):
        w[q] = w[q] - lax.dot_general(bi[q], bj[...], NT, preferred_element_type=F32)
        for pos, fn in stages:
            if nq <= pos < 2 * nq:
                pl.when(q == pos - nq)(fn)

    w_out.start()
    for pos, fn in stages:
        if pos >= 2 * nq:
            fn()
    l_out.wait()
    z_out.wait()
    d_out.wait()
    got("sxp", "sr1lo", "sr1hi", "sr2lo", "sr2hi", "sr3lo", "sr3hi")
    gone("sy+", "sy-", "syf+", "syf-", "sx+lo", "sx+hi", "sx-lo", "sx-hi", "sxp", "sxf+", "sxf-",
         "sr1lo", "sr1hi", "sr2lo", "sr2hi", "sr3lo", "sr3hi")
    w_out.wait()


def fused(a3, sd, s, blk, row_devs, col_devs, nq):
    h = (col_devs // row_devs) * blk
    anyspec = pl.BlockSpec(memory_space=pl.ANY)
    scratch = [
        pltpu.VMEM((col_devs, row_devs, h, blk), F32),
        pltpu.VMEM((blk, blk), F32),
        pltpu.VMEM((col_devs, 3 * blk, 2 * blk), BF16),
        pltpu.VMEM((col_devs * blk, col_devs * blk), BF16),
        pltpu.VMEM((h, nq * blk), F32),
        pltpu.VMEM((col_devs, nq, h + blk, blk), F32),
        pltpu.VMEM((row_devs, h, nq * blk), F32),
        pltpu.VMEM((nq, h, nq * blk), F32),
        pltpu.VMEM((nq, h, col_devs * blk), BF16),
        pltpu.VMEM((nq * blk, col_devs * blk), BF16),
        pltpu.VMEM((h + blk, col_devs * blk), BF16),
        pltpu.VMEM((h, blk), F32),
        pltpu.SemaphoreType.DMA((32,)),
        pltpu.SemaphoreType.DMA((32,)),
        pltpu.SemaphoreType.DMA((8,)),
        pltpu.SemaphoreType.DMA((col_devs,)),
    ]
    return pl.pallas_call(
        functools.partial(fused_kernel, (s, blk, row_devs, col_devs, nq)),
        out_shape=[jax.ShapeDtypeStruct(a3.shape, F32), jax.ShapeDtypeStruct(sd.shape, F32)],
        in_specs=[anyspec, anyspec],
        out_specs=[anyspec, anyspec],
        scratch_shapes=scratch,
        input_output_aliases={} if s == 0 else {0: 0},
        compiler_params=pltpu.CompilerParams(vmem_limit_bytes=60 * 1024 * 1024, collective_id=s + 1, has_side_effects=True),
        name=f"fused_{s}",
    )(a3, sd)


def solution(mesh):
    row_devs = mesh.shape["row"]
    col_devs = mesh.shape["col"]
    per = col_devs // row_devs

    def factor_local(a_loc):
        row_blocks, blk, local_cols = a_loc.shape
        steps = local_cols // blk
        (sd,) = gather(a_loc.reshape(row_blocks * blk, local_cols), 0, blk, row_devs, col_devs, 0, 0)
        a3 = a_loc.reshape(steps, per * blk, local_cols)
        for s in range(steps - 1):
            a3, sd = fused(a3, sd, s, blk, row_devs, col_devs, steps - 1 - s)
        a3 = last(a3, sd, steps - 1, blk, row_devs, col_devs)
        return a3.reshape(row_blocks, blk, local_cols)

    spec = P(("batch", "row"), None, "col")
    return jax.shard_map(factor_local, mesh=mesh, in_specs=(spec,), out_specs=spec, check_vma=False)
```
